32 devices in a mesh: band: 4 (over y, x), ga: 8 (over z, core).
Axes of the slice: x: 2, y: 2, z: 4, core: 2. Of those that a mesh axis runs over, the one named last changes fastest.
Arguments:
- psi: float32 [4096, 4096], P('band', 'ga'), may hold values from -6 to 6
- lower: float32 [4096, 4096], P('band', 'ga'), as said below
Outputs:
- orthonormal: float32 [4096, 4096], P('band', 'ga')
- block_intersection: float32 [4096, 1024], P('band')
The draws below stay inside these ranges and needn't reach their ends.
Inputs may be any that keep to these rules, and one draw needn't show every extreme that they name: lower is lower triangular with its diagonal between 1 and 2.
All inputs are finite; a program needn't handle non-finite values.
Results may differ from the reference program's by a relative error of at most 0.00022.
Values sent between devices are 32-bit elements; how exact they have to be, the bound alone decides.
A program may use at most 64 MiB of HBM per device.

```python
import math
import jax
import jax.numpy as jnp
from jax import lax

NB = 4096
NG = 4096
N_BAND = 4


def draw_lower(key, part):
    first, second = jax.random.split(jax.random.fold_in(key, 11))
    spread = jax.random.normal(first, (NB, NB), jnp.float32) * (2.0 / math.sqrt(NB))
    middle = jax.random.uniform(second, (NB,), jnp.float32, 1.0, 2.0)
    rowpos = lax.broadcasted_iota(jnp.int32, (NB, NB), 0)
    colpos = lax.broadcasted_iota(jnp.int32, (NB, NB), 1)
    return jnp.where(rowpos > colpos, spread, 0.0) + jnp.diag(middle)


def shard_levels(stream_key, extent, pieces, smallest, largest):
    def one(dim, shards_of):
        heights = jax.random.uniform(jax.random.fold_in(jax.random.fold_in(stream_key, 6), dim), (shards_of,), jnp.float32, smallest / len(pieces), largest / len(pieces))
        return jnp.repeat(jnp.exp(heights), extent[dim] // shards_of).reshape((-1,) + (1,) * (len(extent) - dim - 1))

    level = one(*pieces[0])
    for cut in pieces[1:]:
        level = level * one(*cut)
    return level


def bell_draw(key, extent, deviation, bound, shards=(), kind=jnp.bfloat16):
    array = deviation * jax.random.normal(key, extent, jnp.float32)
    if shards:
        array = array * shard_levels(key, extent, shards, -0.22, 0.18)
    return jnp.clip(array, -bound, bound).astype(kind)


def setup_inputs(seed: int = 0) -> dict:
    splits = jax.random.split(jax.random.key(seed), 3)
    psi = bell_draw(splits[0], (NB, NG), 1.0, 6.0, ((0, 4), (1, 8)), jnp.float32)
    lower = draw_lower(jax.random.fold_in(splits[2], 71), 0)
    return {"psi": psi, "lower": lower}


def reference(psi, lower):
    solved = jax.scipy.linalg.solve_triangular(lower, psi, lower=True)
    blocks = solved.reshape(N_BAND, NB // N_BAND, NG)
    intersection = jnp.einsum('bik,bjk->bij', blocks, blocks, precision=lax.Precision.HIGHEST) / NG
    return (solved, intersection.reshape(NB, NB // N_BAND))
```

```python
import functools

import jax
import jax.numpy as jnp
from jax import lax
from jax.experimental import pallas as pl
from jax.experimental.pallas import tpu as pltpu
from jax.sharding import PartitionSpec as P

MESH = pl.DeviceIdType.MESH
BASE = 128
PIECES = 4
CHUNKS = 8
ROWS = 4
F32 = jnp.float32
PAIRS = [(i, j) for i in range(ROWS) for j in range(i + 1)]
SHARE = len(PAIRS) // 2


def split(x):
    high = x.astype(jnp.bfloat16)
    return high, (x - high.astype(F32)).astype(jnp.bfloat16)


def dot(a, b, dims=((1,), (0,)), precision=None):
    return lax.dot_general(a, b, (dims, ((), ())), precision=precision, preferred_element_type=F32)


def mm3(a, b, dims=((1,), (0,))):
    return dot(a[0], b[0], dims) + (dot(a[0], b[1], dims) + dot(a[1], b[0], dims))


def exact(a, b):
    return dot(a, b, precision=lax.Precision.HIGHEST)


def kernel(
    bands, line, psi_ref, low_ref, y_ref, g_ref,
    lbuf, acc, other, own, own_hi, own_lo, part_hi, part_lo, minv, inv_hi, inv_lo, work,
    gpart, gsib, gin, gcross, gout,
    l_recv, l_right, l_left, l_twin, y_recv, y_send, y_out, psi_sem, own_sem,
    twin_sem, gin_recv, cross_recv, in_send, gout_recv, out_send, twin_send,
):
    nrows, width = psi_ref.shape
    lw = low_ref.shape[1]
    rc, w, rb = nrows // CHUNKS, width // PIECES, nrows // ROWS
    b, ga = lax.axis_index("band"), lax.axis_index("ga")
    z, c = ga // 2, ga % 2
    last = bands - 1
    twin = z * 2 + 1 - c

    def remote(src, dst, send, recv, device):
        return pltpu.make_async_remote_copy(
            src_ref=src, dst_ref=dst, send_sem=send, recv_sem=recv,
            device_id=device, device_id_type=MESH,
        )

    def chunk(s, h, i):
        return lbuf.at[s, h, pl.ds(pl.multiple_of(i * rc, rc), rc)]

    def tile_copy(s, i, send, device, h=None):
        h = c if h is None else h
        return remote(chunk(s, h, i), chunk(s, h, i), send.at[s, i], l_recv.at[s, h, i], (b, device))

    def to_right(s, i):
        return tile_copy(s, i, l_right, jnp.minimum(ga + 2, 2 * line - 1))

    def to_left(s, i):
        return tile_copy(s, i, l_left, jnp.maximum(ga - 2, 0))

    def to_twin(s, i):
        return tile_copy(s, i, l_twin, twin)

    def needed(s, h, i):
        return jnp.logical_or(s != b, (i + 1) * rc > h * lw)

    load_own = pltpu.make_async_copy(low_ref, lbuf.at[z, c], own_sem.at[0])
    load_psi = [
        pltpu.make_async_copy(psi_ref.at[:, pl.ds(j * w, w)], acc.at[j], psi_sem.at[j])
        for j in range(PIECES)
    ]

    @pl.when(z <= b)
    def _():
        load_own.start()

    for copy in load_psi:
        copy.start()

    barrier = pltpu.get_barrier_semaphore()
    for device in (lax.rem(ga + 2, 2 * line), lax.rem(ga + 2 * line - 2, 2 * line), twin):
        pl.semaphore_signal(barrier, inc=1, device_id=(b, device), device_id_type=MESH)
    for d in range(1, bands):
        pl.semaphore_signal(barrier, inc=1, device_id=(lax.rem(b + d, bands), ga), device_id_type=MESH)
    pl.semaphore_wait(barrier, 2 + bands)

    @pl.when(z <= b)
    def _():
        load_own.wait()

        @pl.loop(0, CHUNKS)
        def _(i):
            @pl.when(needed(z, c, i))
            def _():
                to_twin(z, i).start()

    def right_tile(turn):
        s = jnp.where(b == last, turn, b if turn == 0 else turn - 1)
        live = jnp.where(b == last, turn < b, turn <= b)
        return s, jnp.logical_and(live, s <= z)

    def left_tile(turn):
        s = b - turn
        return s, s >= z

    def relay(turn, i):
        s, live = right_tile(turn)
        live = jnp.logical_and(live, needed(s, c, i))

        @pl.when(jnp.logical_and(live, s < z))
        def _():
            to_right(s, i).wait_recv()
            to_twin(s, i).start()

        @pl.when(jnp.logical_and(live, z < line - 1))
        def _():
            to_right(s, i).start()

        t, live = left_tile(turn)
        live = jnp.logical_and(live, needed(t, c, i))

        @pl.when(jnp.logical_and(live, t > z))
        def _():
            to_left(t, i).wait_recv()
            to_twin(t, i).start()

        @pl.when(jnp.logical_and(live, z > 0))
        def _():
            to_left(t, i).start()

    def relays(turn, first, count):
        @pl.loop(first, first + count)
        def _(i):
            relay(turn, i)

    def wait_twin(s):
        @pl.loop(0, CHUNKS)
        def _(i):
            @pl.when(needed(s, 1 - c, i))
            def _():
                tile_copy(s, i, l_twin, twin, 1 - c).wait_recv()

    blocks = nrows // BASE
    group = min(4, blocks)

    def invert_blocks(g):
        row = lax.broadcasted_iota(jnp.int32, (BASE, BASE), 0)
        col = lax.broadcasted_iota(jnp.int32, (BASE, BASE), 1)
        tiles, inverses = [], []
        for k in range(group):
            at = (g * group + k) * BASE
            tile = lbuf[b, at // lw, at : at + BASE, at % lw : at % lw + BASE]
            tiles.append(tile)
            inverses.append(jnp.where(row == col, 1.0 / jnp.where(row == col, tile, 1.0), 0.0))
        size = 1
        while size < BASE:
            off = (row // (2 * size) == col // (2 * size)) & (row // size > col // size)
            inner = [exact(jnp.where(off, t, 0.0), v) for t, v in zip(tiles, inverses)]
            inverses = [v - exact(v, u) for v, u in zip(inverses, inner)]
            size *= 2
        for k in range(group):
            at = (g * group + k) * BASE
            minv[at : at + BASE, at : at + BASE] = inverses[k]

    def merge_blocks():
        size = BASE
        while size < nrows:
            step = min(size, 256)
            for at in range(0, nrows, 2 * size):
                half, off = at // lw, at % lw
                first = split(minv[at : at + size, at : at + size])
                for r in range(0, size, step):
                    below = lbuf[b, half, at + size + r : at + size + r + step, off : off + size]
                    work[r : r + step, :size] = mm3(split(below), first)
                inner = split(work[:size, :size])
                for r in range(0, size, step):
                    rows = pl.ds(at + size + r, step)
                    second = minv[rows, at + size : at + 2 * size]
                    minv[rows, at : at + size] = -mm3(split(second), inner)
            size *= 2
        for r in range(ROWS):
            rows, depth = pl.ds(r * rb, rb), (r + 1) * rb
            value = minv[rows, :depth]
            at = lax.broadcasted_iota(jnp.int32, (rb, depth), 0) + r * rb
            value = jnp.where(at >= lax.broadcasted_iota(jnp.int32, (rb, depth), 1), value, 0.0)
            inv_hi[rows, :depth], inv_lo[rows, :depth] = split(value)

    def y_copy(s, j, d):
        return remote(
            own.at[j], other.at[s, j], y_send.at[d - 1, j], y_recv.at[s, j],
            (jnp.minimum(b + d, last), ga),
        )

    def update(s, pieces):
        for j in pieces:
            y_copy(s, j, 1).wait_recv()
            part_hi[j], part_lo[j] = split(other[s, j])

        @pl.loop(0, ROWS)
        def _(r):
            rows = pl.ds(pl.multiple_of(r * rb, rb), rb)
            for h in range(2):
                tile = split(lbuf[s, h, rows])
                for j in pieces:
                    cols = slice(h * lw, (h + 1) * lw)
                    acc[j, rows] -= mm3(tile, (part_hi[j, cols], part_lo[j, cols]))

    def apply_inverse(j):
        part_hi[j], part_lo[j] = split(acc[j])
        for r in range(ROWS):
            rows, depth = slice(r * rb, (r + 1) * rb), (r + 1) * rb
            value = mm3(
                (inv_hi[rows, :depth], inv_lo[rows, :depth]), (part_hi[j, :depth], part_lo[j, :depth])
            )
            own[j, rows] = value
            own_hi[j, rows], own_lo[j, rows] = split(value)

    def out_copy(j):
        return pltpu.make_async_copy(
            own.at[j], y_ref.at[:, pl.ds(pl.multiple_of(j * w, w), w)], y_out.at[j]
        )

    relays(0, 0, CHUNKS)
    wait_twin(b)
    groups = blocks // group
    for g in range(groups):
        relays(1, g * CHUNKS // groups, CHUNKS // groups)
        invert_blocks(g)
    merge_blocks()
    for copy in load_psi:
        copy.wait()
    for turn in range(2, bands - 1):
        if turn == 2:
            @pl.when(b >= 2)
            def _():
                wait_twin(0)
                update(0, range(PIECES))

        relays(turn, 0, CHUNKS)
    for s in range(1, bands - 2):
        @pl.when(b >= s + 2)
        def _():
            wait_twin(s)
            update(s, range(PIECES))

    @pl.when(b > 0)
    def _():
        wait_twin(b - 1)

    gpart[...] = jnp.zeros_like(gpart)

    @pl.loop(0, PIECES)
    def _(j):
        @pl.when(b > 0)
        def _():
            update(b - 1, [j])

        apply_inverse(j)
        for d in range(1, bands):
            @pl.when(b + d < bands)
            def _():
                y_copy(b, j, d).start()

        out_copy(j).start()
        for k, (p, q) in enumerate(PAIRS):
            up, left = slice(p * rb, (p + 1) * rb), slice(q * rb, (q + 1) * rb)
            gpart[k] += mm3(
                (own_hi[j, up], own_lo[j, up]), (own_hi[j, left], own_lo[j, left]), ((1,), (1,))
            )

    mine = c * SHARE
    to_sib = remote(
        gpart.at[pl.ds((1 - c) * SHARE, SHARE)], gsib, twin_sem.at[0], twin_sem.at[1], (b, twin)
    )
    to_sib.start()
    lower_half = z < line // 2
    inward = jnp.where(lower_half, ga + 2, ga - 2)
    has_out = jnp.where(lower_half, z > 0, z < line - 1)
    outward = jnp.where(has_out, jnp.where(lower_half, ga - 2, ga + 2), inward)
    middle = jnp.where(lower_half, z == line // 2 - 1, z == line // 2)

    def in_copy(k):
        return remote(gpart.at[mine + k], gin.at[k], in_send.at[k], gin_recv.at[k], (b, inward))

    def cross_copy(k):
        return remote(gpart.at[mine + k], gcross.at[k], in_send.at[k], cross_recv.at[k], (b, inward))

    def back_copy(k):
        return remote(
            gout.at[mine + k], gout.at[mine + k], out_send.at[k], gout_recv.at[mine + k], (b, outward)
        )

    def share_copy(k, base):
        return remote(
            gout.at[base + k], gout.at[base + k], twin_send.at[k], gout_recv.at[base + k], (b, twin)
        )

    to_sib.wait_recv()

    @pl.loop(0, SHARE)
    def _(k):
        gpart[mine + k] += gsib[k]

        @pl.when(has_out)
        def _():
            in_copy(k).wait_recv()
            gpart[mine + k] += gin[k]

        @pl.when(middle)
        def _():
            cross_copy(k).start()

        @pl.when(jnp.logical_not(middle))
        def _():
            in_copy(k).start()

    @pl.loop(0, SHARE)
    def _(k):
        @pl.when(middle)
        def _():
            cross_copy(k).wait_recv()
            gout[mine + k] = gpart[mine + k] + gcross[k]

        @pl.when(jnp.logical_not(middle))
        def _():
            back_copy(k).wait_recv()

        @pl.when(has_out)
        def _():
            back_copy(k).start()

        share_copy(k, mine).start()

    theirs = (1 - c) * SHARE

    @pl.loop(0, SHARE)
    def _(k):
        share_copy(k, theirs).wait_recv()

    scale = 1.0 / (width * 2 * line)
    for k, (p, q) in enumerate(PAIRS):
        value = gout[k] * scale
        g_ref[p * rb : (p + 1) * rb, q * rb : (q + 1) * rb] = value
        if p != q:
            g_ref[q * rb : (q + 1) * rb, p * rb : (p + 1) * rb] = value.T

    for turn in range(bands - 1):
        @pl.loop(0, CHUNKS)
        def _(i):
            s, live = right_tile(turn)
            live = jnp.logical_and(live, needed(s, c, i))

            @pl.when(jnp.logical_and(live, z < line - 1))
            def _():
                to_right(s, i).wait_send()

            @pl.when(jnp.logical_and(live, s < z))
            def _():
                to_twin(s, i).wait_send()

            t, live = left_tile(turn)
            live = jnp.logical_and(live, needed(t, c, i))

            @pl.when(jnp.logical_and(live, z > 0))
            def _():
                to_left(t, i).wait_send()

            @pl.when(jnp.logical_and(live, t > z))
            def _():
                to_twin(t, i).wait_send()

    @pl.when(z <= b)
    def _():
        @pl.loop(0, CHUNKS)
        def _(i):
            @pl.when(needed(z, c, i))
            def _():
                to_twin(z, i).wait_send()

    @pl.loop(0, PIECES)
    def _(j):
        for d in range(1, bands):
            @pl.when(b + d < bands)
            def _():
                y_copy(b, j, d).wait_send()

        out_copy(j).wait()

    to_sib.wait_send()

    @pl.loop(0, SHARE)
    def _(k):
        in_copy(k).wait_send()
        share_copy(k, mine).wait_send()

        @pl.when(has_out)
        def _():
            back_copy(k).wait_send()


def solution(mesh):
    bands, line = mesh.shape["band"], mesh.shape["ga"] // 2

    def local(psi, lower):
        nrows, width = psi.shape
        lw = lower.shape[1]
        w, rb = width // PIECES, nrows // ROWS
        vmem, dma = pltpu.VMEM, pltpu.SemaphoreType.DMA
        bf16 = jnp.bfloat16
        share = (SHARE, rb, rb)
        return pl.pallas_call(
            functools.partial(kernel, bands, line),
            out_shape=(
                jax.ShapeDtypeStruct((nrows, width), F32),
                jax.ShapeDtypeStruct((nrows, nrows), F32),
            ),
            in_specs=[pl.BlockSpec(memory_space=pl.ANY)] * 2,
            out_specs=(pl.BlockSpec(memory_space=pl.ANY), pl.BlockSpec(memory_space=pltpu.VMEM)),
            scratch_shapes=[
                vmem((bands, 2, nrows, lw), F32),
                vmem((PIECES, nrows, w), F32),
                vmem((bands - 1, PIECES, nrows, w), F32),
                vmem((PIECES, nrows, w), F32),
                vmem((PIECES, nrows, w), bf16),
                vmem((PIECES, nrows, w), bf16),
                vmem((PIECES, nrows, w), bf16),
                vmem((PIECES, nrows, w), bf16),
                vmem((nrows, nrows), F32),
                vmem((nrows, nrows), bf16),
                vmem((nrows, nrows), bf16),
                vmem((nrows // 2, nrows // 2), F32),
                vmem((2 * SHARE, rb, rb), F32),
                vmem(share, F32),
                vmem(share, F32),
                vmem(share, F32),
                vmem((2 * SHARE, rb, rb), F32),
                dma((bands, 2, CHUNKS)),
                dma((bands, CHUNKS)),
                dma((bands, CHUNKS)),
                dma((bands, CHUNKS)),
                dma((bands - 1, PIECES)),
                dma((bands - 1, PIECES)),
                dma((PIECES,)),
                dma((PIECES,)),
                dma((1,)),
                dma((2,)),
                dma((SHARE,)),
                dma((SHARE,)),
                dma((SHARE,)),
                dma((2 * SHARE,)),
                dma((SHARE,)),
                dma((SHARE,)),
            ],
            compiler_params=pltpu.CompilerParams(
                collective_id=0, has_side_effects=True, vmem_limit_bytes=63 * 1024 * 1024
            ),
        )(psi, lower)

    return jax.shard_map(
        local,
        mesh=mesh,
        in_specs=(P("band", "ga"), P("band", "ga")),
        out_specs=(P("band", "ga"), P("band", None)),
        check_vma=False,
    )
```

```python
import functools

import jax
import jax.numpy as jnp
from jax import lax
from jax.experimental import pallas as pl
from jax.experimental.pallas import tpu as pltpu
from jax.sharding import PartitionSpec as P

MESH = pl.DeviceIdType.MESH
BASE = 128
PIECES = 4
CHUNKS = 8
SKEW = 2
ROWS = 4
F32 = jnp.float32
PAIRS = [(i, j) for i in range(ROWS) for j in range(i + 1)]
SHARE = len(PAIRS)


def split(x):
    high = x.astype(jnp.bfloat16)
    return high, (x - high.astype(F32)).astype(jnp.bfloat16)


def dot(a, b, dims=((1,), (0,)), precision=None):
    return lax.dot_general(a, b, (dims, ((), ())), precision=precision, preferred_element_type=F32)


def mm3(a, b, dims=((1,), (0,))):
    return dot(a[0], b[0], dims) + (dot(a[0], b[1], dims) + dot(a[1], b[0], dims))


def exact(a, b):
    return dot(a, b, precision=lax.Precision.HIGHEST)


def kernel(
    bands, line, psi_ref, low_ref, y_ref, g_ref,
    lbuf, acc, other, own, own_hi, own_lo, part_hi, part_lo, minv, inv_hi, inv_lo, work,
    gpart, gsib, gin, gcross, gout,
    l_recv, l_right, l_left, l_twin, y_recv, y_send, y_out, psi_sem, own_sem,
    twin_sem, gin_recv, cross_recv, in_send, gout_recv, out_send, twin_send,
):
    nrows, width = psi_ref.shape
    lw = low_ref.shape[1]
    rc, w, rb = nrows // CHUNKS, width // PIECES, nrows // ROWS
    b, ga = lax.axis_index("band"), lax.axis_index("ga")
    z, c = ga // 2, ga % 2
    last, turns = bands - 1, bands - 1
    drain = SKEW * (line - 1)
    twin = z * 2 + 1 - c

    def remote(src, dst, send, recv, device):
        return pltpu.make_async_remote_copy(
            src_ref=src, dst_ref=dst, send_sem=send, recv_sem=recv,
            device_id=device, device_id_type=MESH,
        )

    def chunk(s, h, i):
        return lbuf.at[s, h, pl.ds(pl.multiple_of(i * rc, rc), rc)]

    def tile_copy(s, i, send, device, h=None):
        h = c if h is None else h
        return remote(chunk(s, h, i), chunk(s, h, i), send.at[s, i], l_recv.at[s, h, i], (b, device))

    def to_right(s, i):
        return tile_copy(s, i, l_right, jnp.minimum(ga + 2, 2 * line - 1))

    def to_left(s, i):
        return tile_copy(s, i, l_left, jnp.maximum(ga - 2, 0))

    def to_twin(s, i):
        return tile_copy(s, i, l_twin, twin)

    def needed(s, h, i):
        return jnp.logical_or(s != b, (i + 1) * rc > h * lw)

    load_own = pltpu.make_async_copy(low_ref, lbuf.at[z, c], own_sem.at[0])
    load_psi = [
        pltpu.make_async_copy(psi_ref.at[:, pl.ds(j * w, w)], acc.at[j], psi_sem.at[j])
        for j in range(PIECES)
    ]

    @pl.when(z <= b)
    def _():
        load_own.start()

    for copy in load_psi:
        copy.start()

    barrier = pltpu.get_barrier_semaphore()
    for device in (lax.rem(ga + 2, 2 * line), lax.rem(ga + 2 * line - 2, 2 * line), twin):
        pl.semaphore_signal(barrier, inc=1, device_id=(b, device), device_id_type=MESH)
    for d in range(1, bands):
        pl.semaphore_signal(barrier, inc=1, device_id=(lax.rem(b + d, bands), ga), device_id_type=MESH)
    pl.semaphore_wait(barrier, 2 + bands)

    @pl.when(z <= b)
    def _():
        load_own.wait()

        @pl.loop(0, CHUNKS)
        def _(i):
            @pl.when(needed(z, c, i))
            def _():
                to_twin(z, i).start()

    def right_tile(turn):
        s = jnp.where(b == last, turn, jnp.where(turn == 0, b, turn - 1))
        live = jnp.where(b == last, turn < b, turn <= b)
        return s, jnp.logical_and(live, s <= z)

    def left_tile(turn):
        s = b - turn
        return s, s >= z

    def stream(tick, hops, tile, moves, send):
        @pl.when(jnp.logical_and(tick >= hops * SKEW, tick < hops * SKEW + turns * CHUNKS))
        def _():
            step = tick - hops * SKEW
            turn, i = step // CHUNKS, step % CHUNKS
            s, live = tile(turn)
            s = jnp.clip(s, 0, last)

            @pl.when(jnp.logical_and(jnp.logical_and(live, s == z), jnp.logical_and(moves, i == 0)))
            def _():
                @pl.loop(0, CHUNKS)
                def _(k):
                    @pl.when(needed(z, c, k))
                    def _():
                        send(z, k).start()

            @pl.when(jnp.logical_and(jnp.logical_and(live, s != z), needed(s, c, i)))
            def _():
                send(s, i).wait_recv()

                @pl.when(moves)
                def _():
                    send(s, i).start()

                to_twin(s, i).start()

    def ticks(first, count):
        @pl.loop(first, first + count)
        def _(tick):
            stream(tick, z, right_tile, z < line - 1, to_right)
            stream(tick, line - 1 - z, left_tile, z > 0, to_left)

    def wait_twin(s):
        @pl.loop(0, CHUNKS)
        def _(i):
            @pl.when(needed(s, 1 - c, i))
            def _():
                tile_copy(s, i, l_twin, twin, 1 - c).wait_recv()

    blocks = nrows // BASE
    group = min(4, blocks)

    def invert_blocks(g):
        row = lax.broadcasted_iota(jnp.int32, (BASE, BASE), 0)
        col = lax.broadcasted_iota(jnp.int32, (BASE, BASE), 1)
        tiles, inverses = [], []
        for k in range(group):
            at = (g * group + k) * BASE
            tile = lbuf[b, at // lw, at : at + BASE, at % lw : at % lw + BASE]
            tiles.append(tile)
            inverses.append(jnp.where(row == col, 1.0 / jnp.where(row == col, tile, 1.0), 0.0))
        size = 1
        while size < BASE:
            off = (row // (2 * size) == col // (2 * size)) & (row // size > col // size)
            inner = [exact(jnp.where(off, t, 0.0), v) for t, v in zip(tiles, inverses)]
            inverses = [v - exact(v, u) for v, u in zip(inverses, inner)]
            size *= 2
        for k in range(group):
            at = (g * group + k) * BASE
            minv[at : at + BASE, at : at + BASE] = inverses[k]

    def merge_blocks():
        size = BASE
        while size < nrows:
            step = min(size, 256)
            for at in range(0, nrows, 2 * size):
                half, off = at // lw, at % lw
                first = split(minv[at : at + size, at : at + size])
                for r in range(0, size, step):
                    below = lbuf[b, half, at + size + r : at + size + r + step, off : off + size]
                    work[r : r + step, :size] = mm3(split(below), first)
                inner = split(work[:size, :size])
                for r in range(0, size, step):
                    rows = pl.ds(at + size + r, step)
                    second = minv[rows, at + size : at + 2 * size]
                    minv[rows, at : at + size] = -mm3(split(second), inner)
            size *= 2
        for r in range(ROWS):
            rows, depth = pl.ds(r * rb, rb), (r + 1) * rb
            value = minv[rows, :depth]
            at = lax.broadcasted_iota(jnp.int32, (rb, depth), 0) + r * rb
            value = jnp.where(at >= lax.broadcasted_iota(jnp.int32, (rb, depth), 1), value, 0.0)
            inv_hi[rows, :depth], inv_lo[rows, :depth] = split(value)

    def y_copy(s, j, d):
        return remote(
            own.at[j], other.at[s, j], y_send.at[d - 1, j], y_recv.at[s, j],
            (jnp.minimum(b + d, last), ga),
        )

    def direct(d):
        reaches = b + d < bands
        return jnp.logical_and(reaches, b > 0) if d == last else reaches

    def pass_on(j):
        return remote(
            other.at[0, j], other.at[0, j], y_send.at[1, j], y_recv.at[0, j], (b * 0 + last, ga)
        )

    def update(s, pieces):
        for j in pieces:
            y_copy(s, j, 1).wait_recv()
            if isinstance(s, int) and s == 0:
                @pl.when(b == last - 1)
                def _():
                    pass_on(j).start()

            part_hi[j], part_lo[j] = split(other[s, j])

        @pl.loop(0, ROWS)
        def _(r):
            rows = pl.ds(pl.multiple_of(r * rb, rb), rb)
            for h in range(2):
                tile = split(lbuf[s, h, rows])
                for j in pieces:
                    cols = slice(h * lw, (h + 1) * lw)
                    acc[j, rows] -= mm3(tile, (part_hi[j, cols], part_lo[j, cols]))

    def apply_inverse(j):
        part_hi[j], part_lo[j] = split(acc[j])
        for r in range(ROWS):
            rows, depth = slice(r * rb, (r + 1) * rb), (r + 1) * rb
            value = mm3(
                (inv_hi[rows, :depth], inv_lo[rows, :depth]), (part_hi[j, :depth], part_lo[j, :depth])
            )
            own[j, rows] = value
            own_hi[j, rows], own_lo[j, rows] = split(value)

    def out_copy(j):
        return pltpu.make_async_copy(
            own.at[j], y_ref.at[:, pl.ds(pl.multiple_of(j * w, w), w)], y_out.at[j]
        )

    ticks(0, CHUNKS + drain)
    wait_twin(b)
    groups = blocks // group
    for g in range(groups):
        ticks(CHUNKS + drain + g * CHUNKS // groups, CHUNKS // groups)
        invert_blocks(g)
    merge_blocks()
    for copy in load_psi:
        copy.wait()
    for turn in range(2, bands - 1):
        if turn == 2:
            @pl.when(b >= 2)
            def _():
                wait_twin(0)
                update(0, range(PIECES))

        ticks(turn * CHUNKS + drain, CHUNKS)
    for s in range(1, bands - 2):
        @pl.when(b >= s + 2)
        def _():
            wait_twin(s)
            update(s, range(PIECES))

    @pl.when(b > 0)
    def _():
        wait_twin(b - 1)

    gpart[...] = jnp.zeros_like(gpart)

    @pl.loop(0, PIECES)
    def _(j):
        @pl.when(b > 0)
        def _():
            update(b - 1, [j])

        apply_inverse(j)
        for d in range(1, bands):
            @pl.when(direct(d))
            def _():
                y_copy(b, j, d).start()

        out_copy(j).start()
        for k, (p, q) in enumerate(PAIRS):
            up, left = slice(p * rb, (p + 1) * rb), slice(q * rb, (q + 1) * rb)
            value = mm3(
                (own_hi[j, up], own_lo[j, up]), (own_hi[j, left], own_lo[j, left]), ((1,), (1,))
            )
            gpart[2 * k] += value[: rb // 2]
            gpart[2 * k + 1] += value[rb // 2 :]

    mine = c * SHARE
    to_sib = remote(
        gpart.at[pl.ds((1 - c) * SHARE, SHARE)], gsib, twin_sem.at[0], twin_sem.at[1], (b, twin)
    )
    to_sib.start()
    lower_half = z < line // 2
    inward = jnp.where(lower_half, ga + 2, ga - 2)
    has_out = jnp.where(lower_half, z > 0, z < line - 1)
    outward = jnp.where(has_out, jnp.where(lower_half, ga - 2, ga + 2), inward)
    middle = jnp.where(lower_half, z == line // 2 - 1, z == line // 2)

    def in_copy(k):
        return remote(gpart.at[mine + k], gin.at[k], in_send.at[k], gin_recv.at[k], (b, inward))

    def cross_copy(k):
        return remote(gpart.at[mine + k], gcross.at[k], in_send.at[k], cross_recv.at[k], (b, inward))

    def back_copy(k):
        return remote(
            gout.at[mine + k], gout.at[mine + k], out_send.at[k], gout_recv.at[mine + k], (b, outward)
        )

    def share_copy(k, base):
        return remote(
            gout.at[base + k], gout.at[base + k], twin_send.at[k], gout_recv.at[base + k], (b, twin)
        )

    to_sib.wait_recv()

    def inward_leg(k):
        gpart[mine + k] += gsib[k]

        @pl.when(has_out)
        def _():
            in_copy(k).wait_recv()
            gpart[mine + k] += gin[k]

        @pl.when(middle)
        def _():
            cross_copy(k).start()

        @pl.when(jnp.logical_not(middle))
        def _():
            in_copy(k).start()

    def outward_leg(k):
        @pl.when(middle)
        def _():
            cross_copy(k).wait_recv()
            gout[mine + k] = gpart[mine + k] + gcross[k]

        @pl.when(jnp.logical_not(middle))
        def _():
            back_copy(k).wait_recv()

        @pl.when(has_out)
        def _():
            back_copy(k).start()

        share_copy(k, mine).start()

    lag = jnp.where(middle, 2, SHARE)

    @pl.loop(0, 2 * SHARE)
    def _(k):
        @pl.when(k < SHARE)
        def _():
            inward_leg(k)

        @pl.when(jnp.logical_and(k >= lag, k < SHARE + lag))
        def _():
            outward_leg(k - lag)

    theirs = (1 - c) * SHARE

    @pl.loop(0, SHARE)
    def _(k):
        share_copy(k, theirs).wait_recv()

    scale = 1.0 / (width * 2 * line)
    for k, (p, q) in enumerate(PAIRS):
        value = jnp.concatenate([gout[2 * k], gout[2 * k + 1]], axis=0) * scale
        g_ref[p * rb : (p + 1) * rb, q * rb : (q + 1) * rb] = value
        if p != q:
            g_ref[q * rb : (q + 1) * rb, p * rb : (p + 1) * rb] = value.T

    for turn in range(bands - 1):
        @pl.loop(0, CHUNKS)
        def _(i):
            s, live = right_tile(turn)
            s = jnp.clip(s, 0, last)
            live = jnp.logical_and(live, needed(s, c, i))

            @pl.when(jnp.logical_and(live, z < line - 1))
            def _():
                to_right(s, i).wait_send()

            @pl.when(jnp.logical_and(live, s < z))
            def _():
                to_twin(s, i).wait_send()

            t, live = left_tile(turn)
            t = jnp.clip(t, 0, last)
            live = jnp.logical_and(live, needed(t, c, i))

            @pl.when(jnp.logical_and(live, z > 0))
            def _():
                to_left(t, i).wait_send()

            @pl.when(jnp.logical_and(live, t > z))
            def _():
                to_twin(t, i).wait_send()

    @pl.when(z <= b)
    def _():
        @pl.loop(0, CHUNKS)
        def _(i):
            @pl.when(needed(z, c, i))
            def _():
                to_twin(z, i).wait_send()

    @pl.loop(0, PIECES)
    def _(j):
        for d in range(1, bands):
            @pl.when(direct(d))
            def _():
                y_copy(b, j, d).wait_send()

        @pl.when(b == last - 1)
        def _():
            pass_on(j).wait_send()

        out_copy(j).wait()

    to_sib.wait_send()

    @pl.loop(0, SHARE)
    def _(k):
        in_copy(k).wait_send()
        share_copy(k, mine).wait_send()

        @pl.when(has_out)
        def _():
            back_copy(k).wait_send()


def solution(mesh):
    bands, line = mesh.shape["band"], mesh.shape["ga"] // 2

    def local(psi, lower):
        nrows, width = psi.shape
        lw = lower.shape[1]
        w, rb = width // PIECES, nrows // ROWS
        vmem, dma = pltpu.VMEM, pltpu.SemaphoreType.DMA
        bf16 = jnp.bfloat16
        share = (SHARE, rb // 2, rb)
        return pl.pallas_call(
            functools.partial(kernel, bands, line),
            out_shape=(
                jax.ShapeDtypeStruct((nrows, width), F32),
                jax.ShapeDtypeStruct((nrows, nrows), F32),
            ),
            in_specs=[pl.BlockSpec(memory_space=pl.ANY)] * 2,
            out_specs=(pl.BlockSpec(memory_space=pl.ANY), pl.BlockSpec(memory_space=pltpu.VMEM)),
            scratch_shapes=[
                vmem((bands, 2, nrows, lw), F32),
                vmem((PIECES, nrows, w), F32),
                vmem((bands - 1, PIECES, nrows, w), F32),
                vmem((PIECES, nrows, w), F32),
                vmem((PIECES, nrows, w), bf16),
                vmem((PIECES, nrows, w), bf16),
                vmem((PIECES, nrows, w), bf16),
                vmem((PIECES, nrows, w), bf16),
                vmem((nrows, nrows), F32),
                vmem((nrows, nrows), bf16),
                vmem((nrows, nrows), bf16),
                vmem((nrows // 2, nrows // 2), F32),
                vmem((2 * SHARE, rb // 2, rb), F32),
                vmem(share, F32),
                vmem(share, F32),
                vmem(share, F32),
                vmem((2 * SHARE, rb // 2, rb), F32),
                dma((bands, 2, CHUNKS)),
                dma((bands, CHUNKS)),
                dma((bands, CHUNKS)),
                dma((bands, CHUNKS)),
                dma((bands - 1, PIECES)),
                dma((bands - 1, PIECES)),
                dma((PIECES,)),
                dma((PIECES,)),
                dma((1,)),
                dma((2,)),
                dma((SHARE,)),
                dma((SHARE,)),
                dma((SHARE,)),
                dma((2 * SHARE,)),
                dma((SHARE,)),
                dma((SHARE,)),
            ],
            compiler_params=pltpu.CompilerParams(
                collective_id=0, has_side_effects=True, vmem_limit_bytes=63 * 1024 * 1024
            ),
        )(psi, lower)

    return jax.shard_map(
        local,
        mesh=mesh,
        in_specs=(P("band", "ga"), P("band", "ga")),
        out_specs=(P("band", "ga"), P("band", None)),
        check_vma=False,
    )
```

```python
import functools

import jax
import jax.numpy as jnp
from jax import lax
from jax.experimental import pallas as pl
from jax.experimental.pallas import tpu as pltpu
from jax.sharding import PartitionSpec as P

MESH = pl.DeviceIdType.MESH
BASE = 128
PIECES = 4
CHUNKS = 8
SKEW = 2
ROWS = 4
F32 = jnp.float32
PAIRS = [(i, j) for i in range(ROWS) for j in range(i + 1)]
SHARE = len(PAIRS)


def split(x):
    high = x.astype(jnp.bfloat16)
    return high, (x - high.astype(F32)).astype(jnp.bfloat16)


def dot(a, b, dims=((1,), (0,))):
    return lax.dot_general(a, b, (dims, ((), ())), preferred_element_type=F32)


def mm3(a, b, dims=((1,), (0,))):
    return dot(a[0], b[0], dims) + (dot(a[0], b[1], dims) + dot(a[1], b[0], dims))


def kernel(
    bands, line, psi_ref, low_ref, y_ref, g_ref,
    lbuf, acc, other, own, own_hi, own_lo, part_hi, part_lo, minv, inv_hi, inv_lo, work,
    gpart, gsib, gin, gcross, gout,
    l_recv, l_right, l_left, l_twin, y_recv, y_send, y_out, psi_sem, own_sem,
    twin_sem, gin_recv, cross_recv, in_send, gout_recv, out_send, twin_send,
):
    nrows, width = psi_ref.shape
    lw = low_ref.shape[1]
    rc, w, rb = nrows // CHUNKS, width // PIECES, nrows // ROWS
    b, ga = lax.axis_index("band"), lax.axis_index("ga")
    z, c = ga // 2, ga % 2
    last, turns = bands - 1, bands - 1
    drain = SKEW * (line - 1)
    twin = z * 2 + 1 - c

    def remote(src, dst, send, recv, device):
        return pltpu.make_async_remote_copy(
            src_ref=src, dst_ref=dst, send_sem=send, recv_sem=recv,
            device_id=device, device_id_type=MESH,
        )

    def chunk(s, h, i):
        return lbuf.at[s, h, pl.ds(pl.multiple_of(i * rc, rc), rc)]

    def tile_copy(s, i, send, device, h=None):
        h = c if h is None else h
        return remote(chunk(s, h, i), chunk(s, h, i), send.at[s, i], l_recv.at[s, h, i], (b, device))

    def to_right(s, i):
        return tile_copy(s, i, l_right, jnp.minimum(ga + 2, 2 * line - 1))

    def to_left(s, i):
        return tile_copy(s, i, l_left, jnp.maximum(ga - 2, 0))

    def to_twin(s, i):
        return tile_copy(s, i, l_twin, twin)

    def needed(s, h, i):
        return jnp.logical_or(s != b, (i + 1) * rc > h * lw)

    load_own = pltpu.make_async_copy(low_ref, lbuf.at[z, c], own_sem.at[0])
    load_psi = [
        pltpu.make_async_copy(psi_ref.at[:, pl.ds(j * w, w)], acc.at[j], psi_sem.at[j])
        for j in range(PIECES)
    ]

    @pl.when(z <= b)
    def _():
        load_own.start()

    for copy in load_psi:
        copy.start()

    barrier = pltpu.get_barrier_semaphore()
    for device in (lax.rem(ga + 2, 2 * line), lax.rem(ga + 2 * line - 2, 2 * line), twin):
        pl.semaphore_signal(barrier, inc=1, device_id=(b, device), device_id_type=MESH)
    for d in range(1, bands):
        pl.semaphore_signal(barrier, inc=1, device_id=(lax.rem(b + d, bands), ga), device_id_type=MESH)
    pl.semaphore_wait(barrier, 2 + bands)

    @pl.when(z <= b)
    def _():
        load_own.wait()

        @pl.loop(0, CHUNKS)
        def _(i):
            @pl.when(needed(z, c, i))
            def _():
                to_twin(z, i).start()

    def right_tile(turn):
        s = jnp.where(b == last, turn, jnp.where(turn == 0, b, turn - 1))
        live = jnp.where(b == last, turn < b, turn <= b)
        return s, jnp.logical_and(live, s <= z)

    def left_tile(turn):
        s = b - turn
        return s, s >= z

    def stream(tick, hops, tile, moves, send):
        @pl.when(jnp.logical_and(tick >= hops * SKEW, tick < hops * SKEW + turns * CHUNKS))
        def _():
            step = tick - hops * SKEW
            turn, i = step // CHUNKS, step % CHUNKS
            s, live = tile(turn)
            s = jnp.clip(s, 0, last)

            @pl.when(jnp.logical_and(jnp.logical_and(live, s == z), jnp.logical_and(moves, i == 0)))
            def _():
                @pl.loop(0, CHUNKS)
                def _(k):
                    @pl.when(needed(z, c, k))
                    def _():
                        send(z, k).start()

            @pl.when(jnp.logical_and(jnp.logical_and(live, s != z), needed(s, c, i)))
            def _():
                send(s, i).wait_recv()

                @pl.when(moves)
                def _():
                    send(s, i).start()

                to_twin(s, i).start()

    def ticks(first, count):
        @pl.loop(first, first + count)
        def _(tick):
            stream(tick, z, right_tile, z < line - 1, to_right)
            stream(tick, line - 1 - z, left_tile, z > 0, to_left)

    def wait_twin(s):
        @pl.loop(0, CHUNKS)
        def _(i):
            @pl.when(needed(s, 1 - c, i))
            def _():
                tile_copy(s, i, l_twin, twin, 1 - c).wait_recv()

    blocks = nrows // BASE
    group = min(4, blocks)

    def invert_blocks(g):
        row = lax.broadcasted_iota(jnp.int32, (BASE, BASE), 0)
        col = lax.broadcasted_iota(jnp.int32, (BASE, BASE), 1)
        tiles, inverses = [], []
        for k in range(group):
            at = (g * group + k) * BASE
            tile = lbuf[b, at // lw, at : at + BASE, at % lw : at % lw + BASE]
            tiles.append(tile)
            inverses.append(jnp.where(row == col, 1.0 / jnp.where(row == col, tile, 1.0), 0.0))
        size = 1
        while size < BASE:
            off = (row // (2 * size) == col // (2 * size)) & (row // size > col // size)
            parts = [split(v) for v in inverses]
            inner = [mm3(split(jnp.where(off, t, 0.0)), v) for t, v in zip(tiles, parts)]
            inverses = [v - mm3(p, split(u)) for v, p, u in zip(inverses, parts, inner)]
            size *= 2
        for k in range(group):
            at = (g * group + k) * BASE
            minv[at : at + BASE, at : at + BASE] = inverses[k]

    def merge_blocks():
        size = BASE
        while size < nrows:
            step = min(size, 256)
            for at in range(0, nrows, 2 * size):
                half, off = at // lw, at % lw
                first = split(minv[at : at + size, at : at + size])
                for r in range(0, size, step):
                    below = lbuf[b, half, at + size + r : at + size + r + step, off : off + size]
                    work[r : r + step, :size] = mm3(split(below), first)
                inner = split(work[:size, :size])
                for r in range(0, size, step):
                    rows = pl.ds(at + size + r, step)
                    second = minv[rows, at + size : at + 2 * size]
                    minv[rows, at : at + size] = -mm3(split(second), inner)
            size *= 2
        for r in range(ROWS):
            rows, depth = pl.ds(r * rb, rb), (r + 1) * rb
            value = minv[rows, :depth]
            at = lax.broadcasted_iota(jnp.int32, (rb, depth), 0) + r * rb
            value = jnp.where(at >= lax.broadcasted_iota(jnp.int32, (rb, depth), 1), value, 0.0)
            inv_hi[rows, :depth], inv_lo[rows, :depth] = split(value)

    def y_copy(s, j, d):
        return remote(
            own.at[j], other.at[s, j], y_send.at[d - 1, j], y_recv.at[s, j],
            (jnp.minimum(b + d, last), ga),
        )

    def direct(d):
        reaches = b + d < bands
        return jnp.logical_and(reaches, b > 0) if d == last else reaches

    def update(s, pieces):
        for j in pieces:
            y_copy(s, j, 1).wait_recv()

            part_hi[j], part_lo[j] = split(other[s, j])

        @pl.loop(0, ROWS)
        def _(r):
            rows = pl.ds(pl.multiple_of(r * rb, rb), rb)
            for h in range(2):
                tile = split(lbuf[s, h, rows])
                for j in pieces:
                    cols = slice(h * lw, (h + 1) * lw)
                    acc[j, rows] -= mm3(tile, (part_hi[j, cols], part_lo[j, cols]))

    def apply_inverse(j):
        part_hi[j], part_lo[j] = split(acc[j])
        for r in range(ROWS):
            rows, depth = slice(r * rb, (r + 1) * rb), (r + 1) * rb
            value = mm3(
                (inv_hi[rows, :depth], inv_lo[rows, :depth]), (part_hi[j, :depth], part_lo[j, :depth])
            )
            own[j, rows] = value
            own_hi[j, rows], own_lo[j, rows] = split(value)

    def out_copy(j):
        return pltpu.make_async_copy(
            own.at[j], y_ref.at[:, pl.ds(pl.multiple_of(j * w, w), w)], y_out.at[j]
        )

    ticks(0, CHUNKS + drain)
    wait_twin(b)
    groups = blocks // group
    for g in range(groups):
        ticks(CHUNKS + drain + g * CHUNKS // groups, CHUNKS // groups)
        invert_blocks(g)
    merge_blocks()
    for copy in load_psi:
        copy.wait()
    for turn in range(2, bands - 1):
        ticks(turn * CHUNKS + drain, CHUNKS)
    @pl.loop(0, b - 1)
    def _(s):
        wait_twin(s)
        update(s, range(PIECES))

    @pl.when(b > 0)
    def _():
        wait_twin(b - 1)

    gpart[...] = jnp.zeros_like(gpart)

    @pl.loop(0, PIECES)
    def _(j):
        @pl.when(b > 0)
        def _():
            update(b - 1, [j])

        apply_inverse(j)
        for d in range(1, bands):
            @pl.when(direct(d))
            def _():
                y_copy(b, j, d).start()

        out_copy(j).start()
        for k, (p, q) in enumerate(PAIRS):
            up, left = slice(p * rb, (p + 1) * rb), slice(q * rb, (q + 1) * rb)
            value = mm3(
                (own_hi[j, up], own_lo[j, up]), (own_hi[j, left], own_lo[j, left]), ((1,), (1,))
            )
            gpart[2 * k] += value[: rb // 2]
            gpart[2 * k + 1] += value[rb // 2 :]

    @pl.when(b == 0)
    def _():
        for j in range(PIECES):
            y_copy(b, j, last).start()

    mine = c * SHARE
    to_sib = remote(
        gpart.at[pl.ds((1 - c) * SHARE, SHARE)], gsib, twin_sem.at[0], twin_sem.at[1], (b, twin)
    )
    to_sib.start()
    lower_half = z < line // 2
    inward = jnp.where(lower_half, ga + 2, ga - 2)
    has_out = jnp.where(lower_half, z > 0, z < line - 1)
    outward = jnp.where(has_out, jnp.where(lower_half, ga - 2, ga + 2), inward)
    middle = jnp.where(lower_half, z == line // 2 - 1, z == line // 2)

    def in_copy(k):
        return remote(gpart.at[mine + k], gin.at[k], in_send.at[k], gin_recv.at[k], (b, inward))

    def cross_copy(k):
        return remote(gpart.at[mine + k], gcross.at[k], in_send.at[k], cross_recv.at[k], (b, inward))

    def back_copy(k):
        return remote(
            gout.at[mine + k], gout.at[mine + k], out_send.at[k], gout_recv.at[mine + k], (b, outward)
        )

    def share_copy(k, base):
        return remote(
            gout.at[base + k], gout.at[base + k], twin_send.at[k], gout_recv.at[base + k], (b, twin)
        )

    to_sib.wait_recv()

    def inward_leg(k):
        gpart[mine + k] += gsib[k]

        @pl.when(has_out)
        def _():
            in_copy(k).wait_recv()
            gpart[mine + k] += gin[k]

        @pl.when(middle)
        def _():
            cross_copy(k).start()

        @pl.when(jnp.logical_not(middle))
        def _():
            in_copy(k).start()

    def outward_leg(k):
        @pl.when(middle)
        def _():
            cross_copy(k).wait_recv()
            gout[mine + k] = gpart[mine + k] + gcross[k]

        @pl.when(jnp.logical_not(middle))
        def _():
            back_copy(k).wait_recv()

        @pl.when(has_out)
        def _():
            back_copy(k).start()

        share_copy(k, mine).start()

    lag = jnp.where(middle, 2, SHARE)

    @pl.loop(0, 2 * SHARE)
    def _(k):
        @pl.when(k < SHARE)
        def _():
            inward_leg(k)

        @pl.when(jnp.logical_and(k >= lag, k < SHARE + lag))
        def _():
            outward_leg(k - lag)

    theirs = (1 - c) * SHARE

    @pl.loop(0, SHARE)
    def _(k):
        share_copy(k, theirs).wait_recv()

    scale = 1.0 / (width * 2 * line)
    for k, (p, q) in enumerate(PAIRS):
        value = jnp.concatenate([gout[2 * k], gout[2 * k + 1]], axis=0) * scale
        g_ref[p * rb : (p + 1) * rb, q * rb : (q + 1) * rb] = value
        if p != q:
            g_ref[q * rb : (q + 1) * rb, p * rb : (p + 1) * rb] = value.T

    for turn in range(bands - 1):
        @pl.loop(0, CHUNKS)
        def _(i):
            s, live = right_tile(turn)
            s = jnp.clip(s, 0, last)
            live = jnp.logical_and(live, needed(s, c, i))

            @pl.when(jnp.logical_and(live, z < line - 1))
            def _():
                to_right(s, i).wait_send()

            @pl.when(jnp.logical_and(live, s < z))
            def _():
                to_twin(s, i).wait_send()

            t, live = left_tile(turn)
            t = jnp.clip(t, 0, last)
            live = jnp.logical_and(live, needed(t, c, i))

            @pl.when(jnp.logical_and(live, z > 0))
            def _():
                to_left(t, i).wait_send()

            @pl.when(jnp.logical_and(live, t > z))
            def _():
                to_twin(t, i).wait_send()

    @pl.when(z <= b)
    def _():
        @pl.loop(0, CHUNKS)
        def _(i):
            @pl.when(needed(z, c, i))
            def _():
                to_twin(z, i).wait_send()

    @pl.loop(0, PIECES)
    def _(j):
        for d in range(1, bands):
            @pl.when(direct(d))
            def _():
                y_copy(b, j, d).wait_send()

        @pl.when(b == 0)
        def _():
            y_copy(b, j, last).wait_send()

        out_copy(j).wait()

    to_sib.wait_send()

    @pl.loop(0, SHARE)
    def _(k):
        in_copy(k).wait_send()
        share_copy(k, mine).wait_send()

        @pl.when(has_out)
        def _():
            back_copy(k).wait_send()


def solution(mesh):
    bands, line = mesh.shape["band"], mesh.shape["ga"] // 2

    def local(psi, lower):
        nrows, width = psi.shape
        lw = lower.shape[1]
        w, rb = width // PIECES, nrows // ROWS
        vmem, dma = pltpu.VMEM, pltpu.SemaphoreType.DMA
        bf16 = jnp.bfloat16
        share = (SHARE, rb // 2, rb)
        return pl.pallas_call(
            functools.partial(kernel, bands, line),
            out_shape=(
                jax.ShapeDtypeStruct((nrows, width), F32),
                jax.ShapeDtypeStruct((nrows, nrows), F32),
            ),
            in_specs=[pl.BlockSpec(memory_space=pl.ANY)] * 2,
            out_specs=(pl.BlockSpec(memory_space=pl.ANY), pl.BlockSpec(memory_space=pltpu.VMEM)),
            scratch_shapes=[
                vmem((bands, 2, nrows, lw), F32),
                vmem((PIECES, nrows, w), F32),
                vmem((bands - 1, PIECES, nrows, w), F32),
                vmem((PIECES, nrows, w), F32),
                vmem((PIECES, nrows, w), bf16),
                vmem((PIECES, nrows, w), bf16),
                vmem((PIECES, nrows, w), bf16),
                vmem((PIECES, nrows, w), bf16),
                vmem((nrows, nrows), F32),
                vmem((nrows, nrows), bf16),
                vmem((nrows, nrows), bf16),
                vmem((nrows // 2, nrows // 2), F32),
                vmem((2 * SHARE, rb // 2, rb), F32),
                vmem(share, F32),
                vmem(share, F32),
                vmem(share, F32),
                vmem((2 * SHARE, rb // 2, rb), F32),
                dma((bands, 2, CHUNKS)),
                dma((bands, CHUNKS)),
                dma((bands, CHUNKS)),
                dma((bands, CHUNKS)),
                dma((bands - 1, PIECES)),
                dma((bands - 1, PIECES)),
                dma((PIECES,)),
                dma((PIECES,)),
                dma((1,)),
                dma((2,)),
                dma((SHARE,)),
                dma((SHARE,)),
                dma((SHARE,)),
                dma((2 * SHARE,)),
                dma((SHARE,)),
                dma((SHARE,)),
            ],
            compiler_params=pltpu.CompilerParams(
                collective_id=0, has_side_effects=True, vmem_limit_bytes=63 * 1024 * 1024
            ),
        )(psi, lower)

    return jax.shard_map(
        local,
        mesh=mesh,
        in_specs=(P("band", "ga"), P("band", "ga")),
        out_specs=(P("band", "ga"), P("band", None)),
        check_vma=False,
    )
```

```python
import functools

import jax
import jax.numpy as jnp
from jax import lax
from jax.experimental import pallas as pl
from jax.experimental.pallas import tpu as pltpu
from jax.sharding import PartitionSpec as P

MESH = pl.DeviceIdType.MESH
BASE = 128
PIECES = 4
CHUNKS = 8
SKEW = 2
ROWS = 4
F32 = jnp.float32
PAIRS = [(i, j) for i in range(ROWS) for j in range(i + 1)]
SHARE = len(PAIRS)


def split(x):
    high = x.astype(jnp.bfloat16)
    return high, (x - high.astype(F32)).astype(jnp.bfloat16)


def dot(a, b, dims=((1,), (0,))):
    return lax.dot_general(a, b, (dims, ((), ())), preferred_element_type=F32)


def mm3(a, b, dims=((1,), (0,))):
    return dot(a[0], b[0], dims) + (dot(a[0], b[1], dims) + dot(a[1], b[0], dims))


def kernel(
    bands, line, psi_ref, low_ref, y_ref, g_ref,
    lbuf, acc, other, own, own_hi, own_lo, part_hi, part_lo, minv, inv_hi, inv_lo, work,
    gpart, gsib, gin, gcross, gout,
    l_recv, l_right, l_left, l_twin, y_recv, y_send, y_out, psi_sem, own_sem,
    twin_sem, gin_recv, cross_recv, in_send, gout_recv, out_send, twin_send,
):
    nrows, width = psi_ref.shape
    lw = low_ref.shape[1]
    rc, w, rb = nrows // CHUNKS, width // PIECES, nrows // ROWS
    b, ga = lax.axis_index("band"), lax.axis_index("ga")
    z, c = ga // 2, ga % 2
    last, turns = bands - 1, bands - 1
    drain = SKEW * (line - 1)
    twin = z * 2 + 1 - c

    def remote(src, dst, send, recv, device):
        return pltpu.make_async_remote_copy(
            src_ref=src, dst_ref=dst, send_sem=send, recv_sem=recv,
            device_id=device, device_id_type=MESH,
        )

    def chunk(s, h, i, wide):
        rows = pl.ds(pl.multiple_of(i * rc, rc), rc)
        return lbuf.at[s, h, rows, pl.ds(0, wide)]

    def tile_copy(s, i, send, device, wide, h=None):
        h = c if h is None else h
        part = chunk(s, h, i, wide)
        return remote(part, part, send.at[s, i], l_recv.at[s, h, i], (b, device))

    def to_right(s, i, wide):
        return tile_copy(s, i, l_right, jnp.minimum(ga + 2, 2 * line - 1), wide)

    def to_left(s, i, wide):
        return tile_copy(s, i, l_left, jnp.maximum(ga - 2, 0), wide)

    def to_twin(s, i, wide):
        return tile_copy(s, i, l_twin, twin, wide)

    def sizes(s, h, i, on=True):
        lanes = 128
        reach = jnp.minimum(((i + 1) * rc - h * lw + lanes - 1) // lanes, lw // lanes)
        count = jnp.where(s == b, reach, lw // lanes)
        return [(m * lanes, jnp.logical_and(on, count == m)) for m in range(1, lw // lanes + 1)]

    load_own = pltpu.make_async_copy(low_ref, lbuf.at[z, c], own_sem.at[0])
    load_psi = [
        pltpu.make_async_copy(psi_ref.at[:, pl.ds(j * w, w)], acc.at[j], psi_sem.at[j])
        for j in range(PIECES)
    ]

    @pl.when(z <= b)
    def _():
        load_own.start()

    for copy in load_psi:
        copy.start()

    barrier = pltpu.get_barrier_semaphore()
    for device in (lax.rem(ga + 2, 2 * line), lax.rem(ga + 2 * line - 2, 2 * line), twin):
        pl.semaphore_signal(barrier, inc=1, device_id=(b, device), device_id_type=MESH)
    for d in range(1, bands):
        pl.semaphore_signal(barrier, inc=1, device_id=(lax.rem(b + d, bands), ga), device_id_type=MESH)
    pl.semaphore_wait(barrier, 2 + bands)

    @pl.when(z <= b)
    def _():
        load_own.wait()

        @pl.loop(0, CHUNKS)
        def _(i):
            for wide, on in sizes(z, c, i):
                @pl.when(on)
                def _():
                    to_twin(z, i, wide).start()

    def right_tile(turn):
        s = jnp.where(b == last, turn, jnp.where(turn == 0, b, turn - 1))
        live = jnp.where(b == last, turn < b, turn <= b)
        return s, jnp.logical_and(live, s <= z)

    def left_tile(turn):
        s = b - turn
        return s, s >= z

    def stream(tick, hops, tile, moves, send):
        @pl.when(jnp.logical_and(tick >= hops * SKEW, tick < hops * SKEW + turns * CHUNKS))
        def _():
            step = tick - hops * SKEW
            turn, i = step // CHUNKS, step % CHUNKS
            s, live = tile(turn)
            s = jnp.clip(s, 0, last)

            @pl.when(jnp.logical_and(jnp.logical_and(live, s == z), jnp.logical_and(moves, i == 0)))
            def _():
                @pl.loop(0, CHUNKS)
                def _(k):
                    for wide, on in sizes(z, c, k):
                        @pl.when(on)
                        def _():
                            send(z, k, wide).start()

            for wide, on in sizes(s, c, i, jnp.logical_and(live, s != z)):
                @pl.when(on)
                def _():
                    send(s, i, wide).wait_recv()

                    @pl.when(moves)
                    def _():
                        send(s, i, wide).start()

                    to_twin(s, i, wide).start()

    def ticks(first, count):
        @pl.loop(first, first + count)
        def _(tick):
            stream(tick, z, right_tile, z < line - 1, to_right)
            stream(tick, line - 1 - z, left_tile, z > 0, to_left)

    def wait_twin(s):
        @pl.loop(0, CHUNKS)
        def _(i):
            for wide, on in sizes(s, 1 - c, i):
                @pl.when(on)
                def _():
                    tile_copy(s, i, l_twin, twin, wide, 1 - c).wait_recv()

    blocks = nrows // BASE
    group = min(4, blocks)

    def invert_blocks(g):
        row = lax.broadcasted_iota(jnp.int32, (BASE, BASE), 0)
        col = lax.broadcasted_iota(jnp.int32, (BASE, BASE), 1)
        tiles, inverses = [], []
        for k in range(group):
            at = (g * group + k) * BASE
            tile = lbuf[b, at // lw, at : at + BASE, at % lw : at % lw + BASE]
            tiles.append(tile)
            inverses.append(jnp.where(row == col, 1.0 / jnp.where(row == col, tile, 1.0), 0.0))
        size = 1
        while size < BASE:
            off = (row // (2 * size) == col // (2 * size)) & (row // size > col // size)
            parts = [split(v) for v in inverses]
            inner = [mm3(split(jnp.where(off, t, 0.0)), v) for t, v in zip(tiles, parts)]
            inverses = [v - mm3(p, split(u)) for v, p, u in zip(inverses, parts, inner)]
            size *= 2
        for k in range(group):
            at = (g * group + k) * BASE
            minv[at : at + BASE, at : at + BASE] = inverses[k]

    def merge_blocks():
        size = BASE
        while size < nrows:
            step = min(size, 256)
            for at in range(0, nrows, 2 * size):
                half, off = at // lw, at % lw
                first = split(minv[at : at + size, at : at + size])
                for r in range(0, size, step):
                    below = lbuf[b, half, at + size + r : at + size + r + step, off : off + size]
                    work[r : r + step, :size] = mm3(split(below), first)
                inner = split(work[:size, :size])
                for r in range(0, size, step):
                    rows = pl.ds(at + size + r, step)
                    second = minv[rows, at + size : at + 2 * size]
                    minv[rows, at : at + size] = -mm3(split(second), inner)
            size *= 2
        for r in range(ROWS):
            rows, depth = pl.ds(r * rb, rb), (r + 1) * rb
            value = minv[rows, :depth]
            at = lax.broadcasted_iota(jnp.int32, (rb, depth), 0) + r * rb
            value = jnp.where(at >= lax.broadcasted_iota(jnp.int32, (rb, depth), 1), value, 0.0)
            inv_hi[rows, :depth], inv_lo[rows, :depth] = split(value)

    def y_copy(s, j, d):
        return remote(
            own.at[j], other.at[s, j], y_send.at[d - 1, j], y_recv.at[s, j],
            (jnp.minimum(b + d, last), ga),
        )

    def direct(d):
        reaches = b + d < bands
        return jnp.logical_and(reaches, b > 0) if d == last else reaches

    def update(s, pieces):
        for j in pieces:
            y_copy(s, j, 1).wait_recv()

            part_hi[j], part_lo[j] = split(other[s, j])

        @pl.loop(0, ROWS)
        def _(r):
            rows = pl.ds(pl.multiple_of(r * rb, rb), rb)
            for h in range(2):
                tile = split(lbuf[s, h, rows])
                for j in pieces:
                    cols = slice(h * lw, (h + 1) * lw)
                    acc[j, rows] -= mm3(tile, (part_hi[j, cols], part_lo[j, cols]))

    def apply_inverse(j):
        part_hi[j], part_lo[j] = split(acc[j])
        for r in range(ROWS):
            rows, depth = slice(r * rb, (r + 1) * rb), (r + 1) * rb
            value = mm3(
                (inv_hi[rows, :depth], inv_lo[rows, :depth]), (part_hi[j, :depth], part_lo[j, :depth])
            )
            own[j, rows] = value
            own_hi[j, rows], own_lo[j, rows] = split(value)

    def out_copy(j):
        return pltpu.make_async_copy(
            own.at[j], y_ref.at[:, pl.ds(pl.multiple_of(j * w, w), w)], y_out.at[j]
        )

    ticks(0, CHUNKS + drain)
    wait_twin(b)
    groups = blocks // group
    for g in range(groups):
        ticks(CHUNKS + drain + g * CHUNKS // groups, CHUNKS // groups)
        invert_blocks(g)
    merge_blocks()
    for copy in load_psi:
        copy.wait()
    for turn in range(2, bands - 1):
        ticks(turn * CHUNKS + drain, CHUNKS)
    @pl.when(b >= 2)
    def _():
        wait_twin(0)
        update(0, range(PIECES))

    fresh = jnp.where(b >= 2, 1, 0)

    @pl.loop(fresh, b)
    def _(s):
        wait_twin(s)

    gpart[...] = jnp.zeros_like(gpart)

    @pl.loop(0, PIECES)
    def _(j):
        @pl.loop(fresh, b)
        def _(s):
            update(s, [j])

        apply_inverse(j)
        for d in range(1, bands):
            @pl.when(direct(d))
            def _():
                y_copy(b, j, d).start()

        out_copy(j).start()
        for k, (p, q) in enumerate(PAIRS):
            up, left = slice(p * rb, (p + 1) * rb), slice(q * rb, (q + 1) * rb)
            value = mm3(
                (own_hi[j, up], own_lo[j, up]), (own_hi[j, left], own_lo[j, left]), ((1,), (1,))
            )
            gpart[2 * k] += value[: rb // 2]
            gpart[2 * k + 1] += value[rb // 2 :]

    @pl.when(b == 0)
    def _():
        for j in range(PIECES):
            y_copy(b, j, last).start()

    mine = c * SHARE
    to_sib = remote(
        gpart.at[pl.ds((1 - c) * SHARE, SHARE)], gsib, twin_sem.at[0], twin_sem.at[1], (b, twin)
    )
    to_sib.start()
    lower_half = z < line // 2
    inward = jnp.where(lower_half, ga + 2, ga - 2)
    has_out = jnp.where(lower_half, z > 0, z < line - 1)
    outward = jnp.where(has_out, jnp.where(lower_half, ga - 2, ga + 2), inward)
    middle = jnp.where(lower_half, z == line // 2 - 1, z == line // 2)

    def in_copy(k):
        return remote(gpart.at[mine + k], gin.at[k], in_send.at[k], gin_recv.at[k], (b, inward))

    def cross_copy(k):
        return remote(gpart.at[mine + k], gcross.at[k], in_send.at[k], cross_recv.at[k], (b, inward))

    def back_copy(k):
        return remote(
            gout.at[mine + k], gout.at[mine + k], out_send.at[k], gout_recv.at[mine + k], (b, outward)
        )

    def share_copy(k, base):
        return remote(
            gout.at[base + k], gout.at[base + k], twin_send.at[k], gout_recv.at[base + k], (b, twin)
        )

    to_sib.wait_recv()

    def inward_leg(k):
        gpart[mine + k] += gsib[k]

        @pl.when(has_out)
        def _():
            in_copy(k).wait_recv()
            gpart[mine + k] += gin[k]

        @pl.when(middle)
        def _():
            cross_copy(k).start()

        @pl.when(jnp.logical_not(middle))
        def _():
            in_copy(k).start()

    def outward_leg(k):
        @pl.when(middle)
        def _():
            cross_copy(k).wait_recv()
            gout[mine + k] = gpart[mine + k] + gcross[k]

        @pl.when(jnp.logical_not(middle))
        def _():
            back_copy(k).wait_recv()

        @pl.when(has_out)
        def _():
            back_copy(k).start()

        share_copy(k, mine).start()

    lag = jnp.where(middle, 2, SHARE)

    @pl.loop(0, 2 * SHARE)
    def _(k):
        @pl.when(k < SHARE)
        def _():
            inward_leg(k)

        @pl.when(jnp.logical_and(k >= lag, k < SHARE + lag))
        def _():
            outward_leg(k - lag)

    theirs = (1 - c) * SHARE

    @pl.loop(0, SHARE)
    def _(k):
        share_copy(k, theirs).wait_recv()

    scale = 1.0 / (width * 2 * line)
    for k, (p, q) in enumerate(PAIRS):
        value = jnp.concatenate([gout[2 * k], gout[2 * k + 1]], axis=0) * scale
        g_ref[p * rb : (p + 1) * rb, q * rb : (q + 1) * rb] = value
        if p != q:
            g_ref[q * rb : (q + 1) * rb, p * rb : (p + 1) * rb] = value.T

    def drained(tile, turn, i, moves, send):
        s, live = tile(turn)
        s = jnp.clip(s, 0, last)
        for wide, on in sizes(s, c, i, live):
            @pl.when(jnp.logical_and(on, moves))
            def _():
                send(s, i, wide).wait_send()

            @pl.when(jnp.logical_and(on, s != z))
            def _():
                to_twin(s, i, wide).wait_send()

    for turn in range(bands - 1):
        @pl.loop(0, CHUNKS)
        def _(i):
            drained(right_tile, turn, i, z < line - 1, to_right)
            drained(left_tile, turn, i, z > 0, to_left)

    @pl.when(z <= b)
    def _():
        @pl.loop(0, CHUNKS)
        def _(i):
            for wide, on in sizes(z, c, i):
                @pl.when(on)
                def _():
                    to_twin(z, i, wide).wait_send()

    @pl.loop(0, PIECES)
    def _(j):
        for d in range(1, bands):
            @pl.when(direct(d))
            def _():
                y_copy(b, j, d).wait_send()

        @pl.when(b == 0)
        def _():
            y_copy(b, j, last).wait_send()

        out_copy(j).wait()

    to_sib.wait_send()

    @pl.loop(0, SHARE)
    def _(k):
        in_copy(k).wait_send()
        share_copy(k, mine).wait_send()

        @pl.when(has_out)
        def _():
            back_copy(k).wait_send()


def solution(mesh):
    bands, line = mesh.shape["band"], mesh.shape["ga"] // 2

    def local(psi, lower):
        nrows, width = psi.shape
        lw = lower.shape[1]
        w, rb = width // PIECES, nrows // ROWS
        vmem, dma = pltpu.VMEM, pltpu.SemaphoreType.DMA
        bf16 = jnp.bfloat16
        share = (SHARE, rb // 2, rb)
        return pl.pallas_call(
            functools.partial(kernel, bands, line),
            out_shape=(
                jax.ShapeDtypeStruct((nrows, width), F32),
                jax.ShapeDtypeStruct((nrows, nrows), F32),
            ),
            in_specs=[pl.BlockSpec(memory_space=pl.ANY)] * 2,
            out_specs=(pl.BlockSpec(memory_space=pl.ANY), pl.BlockSpec(memory_space=pltpu.VMEM)),
            scratch_shapes=[
                vmem((bands, 2, nrows, lw), F32),
                vmem((PIECES, nrows, w), F32),
                vmem((bands - 1, PIECES, nrows, w), F32),
                vmem((PIECES, nrows, w), F32),
                vmem((PIECES, nrows, w), bf16),
                vmem((PIECES, nrows, w), bf16),
                vmem((PIECES, nrows, w), bf16),
                vmem((PIECES, nrows, w), bf16),
                vmem((nrows, nrows), F32),
                vmem((nrows, nrows), bf16),
                vmem((nrows, nrows), bf16),
                vmem((nrows // 2, nrows // 2), F32),
                vmem((2 * SHARE, rb // 2, rb), F32),
                vmem(share, F32),
                vmem(share, F32),
                vmem(share, F32),
                vmem((2 * SHARE, rb // 2, rb), F32),
                dma((bands, 2, CHUNKS)),
                dma((bands, CHUNKS)),
                dma((bands, CHUNKS)),
                dma((bands, CHUNKS)),
                dma((bands - 1, PIECES)),
                dma((bands - 1, PIECES)),
                dma((PIECES,)),
                dma((PIECES,)),
                dma((1,)),
                dma((2,)),
                dma((SHARE,)),
                dma((SHARE,)),
                dma((SHARE,)),
                dma((2 * SHARE,)),
                dma((SHARE,)),
                dma((SHARE,)),
            ],
            compiler_params=pltpu.CompilerParams(
                collective_id=0, has_side_effects=True, vmem_limit_bytes=63 * 1024 * 1024
            ),
        )(psi, lower)

    return jax.shard_map(
        local,
        mesh=mesh,
        in_specs=(P("band", "ga"), P("band", "ga")),
        out_specs=(P("band", "ga"), P("band", None)),
        check_vma=False,
    )
```

```python
import functools

import jax
import jax.numpy as jnp
from jax import lax
from jax.experimental import pallas as pl
from jax.experimental.pallas import tpu as pltpu
from jax.sharding import PartitionSpec as P

MESH = pl.DeviceIdType.MESH
BASE = 128
PIECES = 4
CHUNKS = 16
SKEW = 2
ROWS = 4
F32 = jnp.float32
PAIRS = [(i, j) for i in range(ROWS) for j in range(i + 1)]
SHARE = len(PAIRS)


def split(x):
    high = x.astype(jnp.bfloat16)
    return high, (x - high.astype(F32)).astype(jnp.bfloat16)


def dot(a, b, dims=((1,), (0,))):
    return lax.dot_general(a, b, (dims, ((), ())), preferred_element_type=F32)


def mm3(a, b, dims=((1,), (0,))):
    return dot(a[0], b[0], dims) + (dot(a[0], b[1], dims) + dot(a[1], b[0], dims))


def kernel(
    bands, line, psi_ref, low_ref, y_ref, g_ref,
    lbuf, acc, other, own, own_hi, own_lo, part_hi, part_lo, minv, inv_hi, inv_lo, work,
    gpart, gsib, gin, gcross, gout,
    l_recv, l_right, l_left, l_twin, y_recv, y_send, y_out, psi_sem, own_sem,
    twin_sem, gin_recv, cross_recv, in_send, gout_recv, out_send, twin_send,
):
    nrows, width = psi_ref.shape
    lw = low_ref.shape[1]
    rc, w, rb = nrows // CHUNKS, width // PIECES, nrows // ROWS
    b, ga = lax.axis_index("band"), lax.axis_index("ga")
    z, c = ga // 2, ga % 2
    last, turns = bands - 1, bands - 1
    drain = SKEW * (line - 1)
    twin = z * 2 + 1 - c

    def remote(src, dst, send, recv, device):
        return pltpu.make_async_remote_copy(
            src_ref=src, dst_ref=dst, send_sem=send, recv_sem=recv,
            device_id=device, device_id_type=MESH,
        )

    def chunk(s, h, i, wide):
        rows = pl.ds(pl.multiple_of(i * rc, rc), rc)
        return lbuf.at[s, h, rows, pl.ds(0, wide)]

    def tile_copy(s, i, send, device, wide, h=None):
        h = c if h is None else h
        part = chunk(s, h, i, wide)
        return remote(part, part, send.at[s, i], l_recv.at[s, h, i], (b, device))

    def to_right(s, i, wide):
        return tile_copy(s, i, l_right, jnp.minimum(ga + 2, 2 * line - 1), wide)

    def to_left(s, i, wide):
        return tile_copy(s, i, l_left, jnp.maximum(ga - 2, 0), wide)

    def to_twin(s, i, wide):
        return tile_copy(s, i, l_twin, twin, wide)

    def sizes(s, h, i, on=True):
        lanes = 128
        reach = jnp.minimum(((i + 1) * rc - h * lw + lanes - 1) // lanes, lw // lanes)
        count = jnp.where(s == b, reach, lw // lanes)
        return [(m * lanes, jnp.logical_and(on, count == m)) for m in range(1, lw // lanes + 1)]

    load_own = pltpu.make_async_copy(low_ref, lbuf.at[z, c], own_sem.at[0])
    load_psi = [
        pltpu.make_async_copy(psi_ref.at[:, pl.ds(j * w, w)], acc.at[j], psi_sem.at[j])
        for j in range(PIECES)
    ]

    @pl.when(z <= b)
    def _():
        load_own.start()

    for copy in load_psi:
        copy.start()

    barrier = pltpu.get_barrier_semaphore()
    for device in (lax.rem(ga + 2, 2 * line), lax.rem(ga + 2 * line - 2, 2 * line), twin):
        pl.semaphore_signal(barrier, inc=1, device_id=(b, device), device_id_type=MESH)
    for d in range(1, bands):
        pl.semaphore_signal(barrier, inc=1, device_id=(lax.rem(b + d, bands), ga), device_id_type=MESH)
    pl.semaphore_wait(barrier, 2 + bands)

    @pl.when(z <= b)
    def _():
        load_own.wait()

        @pl.loop(0, CHUNKS)
        def _(i):
            for wide, on in sizes(z, c, i):
                @pl.when(on)
                def _():
                    to_twin(z, i, wide).start()

    def right_tile(turn):
        s = jnp.where(b == last, turn, jnp.where(turn == 0, b, turn - 1))
        live = jnp.where(b == last, turn < b, turn <= b)
        return s, jnp.logical_and(live, s <= z)

    def left_tile(turn):
        s = b - turn
        return s, s >= z

    def stream(tick, hops, tile, moves, send):
        @pl.when(jnp.logical_and(tick >= hops * SKEW, tick < hops * SKEW + turns * CHUNKS))
        def _():
            step = tick - hops * SKEW
            turn, i = step // CHUNKS, step % CHUNKS
            s, live = tile(turn)
            s = jnp.clip(s, 0, last)

            @pl.when(jnp.logical_and(jnp.logical_and(live, s == z), jnp.logical_and(moves, i == 0)))
            def _():
                @pl.loop(0, CHUNKS)
                def _(k):
                    for wide, on in sizes(z, c, k):
                        @pl.when(on)
                        def _():
                            send(z, k, wide).start()

            for wide, on in sizes(s, c, i, jnp.logical_and(live, s != z)):
                @pl.when(on)
                def _():
                    send(s, i, wide).wait_recv()

                    @pl.when(moves)
                    def _():
                        send(s, i, wide).start()

                    to_twin(s, i, wide).start()

    def ticks(first, count):
        @pl.loop(first, first + count)
        def _(tick):
            stream(tick, z, right_tile, z < line - 1, to_right)
            stream(tick, line - 1 - z, left_tile, z > 0, to_left)

    def wait_twin(s):
        @pl.loop(0, CHUNKS)
        def _(i):
            for wide, on in sizes(s, 1 - c, i):
                @pl.when(on)
                def _():
                    tile_copy(s, i, l_twin, twin, wide, 1 - c).wait_recv()

    blocks = nrows // BASE
    group = min(4, blocks)

    def invert_blocks(g):
        row = lax.broadcasted_iota(jnp.int32, (BASE, BASE), 0)
        col = lax.broadcasted_iota(jnp.int32, (BASE, BASE), 1)
        tiles, inverses = [], []
        for k in range(group):
            at = (g * group + k) * BASE
            tile = lbuf[b, at // lw, at : at + BASE, at % lw : at % lw + BASE]
            tiles.append(tile)
            inverses.append(jnp.where(row == col, 1.0 / jnp.where(row == col, tile, 1.0), 0.0))
        size = 1
        while size < BASE:
            off = (row // (2 * size) == col // (2 * size)) & (row // size > col // size)
            parts = [split(v) for v in inverses]
            inner = [mm3(split(jnp.where(off, t, 0.0)), v) for t, v in zip(tiles, parts)]
            inverses = [v - mm3(p, split(u)) for v, p, u in zip(inverses, parts, inner)]
            size *= 2
        for k in range(group):
            at = (g * group + k) * BASE
            minv[at : at + BASE, at : at + BASE] = inverses[k]

    def merge_blocks():
        size = BASE
        while size < nrows:
            step = min(size, 256)
            for at in range(0, nrows, 2 * size):
                half, off = at // lw, at % lw
                first = split(minv[at : at + size, at : at + size])
                for r in range(0, size, step):
                    below = lbuf[b, half, at + size + r : at + size + r + step, off : off + size]
                    work[r : r + step, :size] = mm3(split(below), first)
                inner = split(work[:size, :size])
                for r in range(0, size, step):
                    rows = pl.ds(at + size + r, step)
                    second = minv[rows, at + size : at + 2 * size]
                    minv[rows, at : at + size] = -mm3(split(second), inner)
            size *= 2
        for r in range(ROWS):
            rows, depth = pl.ds(r * rb, rb), (r + 1) * rb
            value = minv[rows, :depth]
            at = lax.broadcasted_iota(jnp.int32, (rb, depth), 0) + r * rb
            value = jnp.where(at >= lax.broadcasted_iota(jnp.int32, (rb, depth), 1), value, 0.0)
            inv_hi[rows, :depth], inv_lo[rows, :depth] = split(value)

    def y_copy(s, j, d):
        return remote(
            own.at[j], other.at[s, j], y_send.at[d - 1, j], y_recv.at[s, j],
            (jnp.minimum(b + d, last), ga),
        )

    def direct(d):
        reaches = b + d < bands
        return jnp.logical_and(reaches, b > 0) if d == last else reaches

    def update(s, pieces):
        for j in pieces:
            y_copy(s, j, 1).wait_recv()

            part_hi[j], part_lo[j] = split(other[s, j])

        @pl.loop(0, ROWS)
        def _(r):
            rows = pl.ds(pl.multiple_of(r * rb, rb), rb)
            for h in range(2):
                tile = split(lbuf[s, h, rows])
                for j in pieces:
                    cols = slice(h * lw, (h + 1) * lw)
                    acc[j, rows] -= mm3(tile, (part_hi[j, cols], part_lo[j, cols]))

    def apply_inverse(j):
        part_hi[j], part_lo[j] = split(acc[j])
        for r in range(ROWS):
            rows, depth = slice(r * rb, (r + 1) * rb), (r + 1) * rb
            value = mm3(
                (inv_hi[rows, :depth], inv_lo[rows, :depth]), (part_hi[j, :depth], part_lo[j, :depth])
            )
            own[j, rows] = value
            own_hi[j, rows], own_lo[j, rows] = split(value)

    def out_copy(j):
        return pltpu.make_async_copy(
            own.at[j], y_ref.at[:, pl.ds(pl.multiple_of(j * w, w), w)], y_out.at[j]
        )

    ticks(0, CHUNKS + drain)
    wait_twin(b)
    groups = blocks // group
    for g in range(groups):
        ticks(CHUNKS + drain + g * CHUNKS // groups, CHUNKS // groups)
        invert_blocks(g)
    merge_blocks()
    for copy in load_psi:
        copy.wait()
    for turn in range(2, bands - 1):
        ticks(turn * CHUNKS + drain, CHUNKS)
    @pl.when(b >= 2)
    def _():
        wait_twin(0)
        update(0, range(PIECES))

    fresh = jnp.where(b >= 2, 1, 0)

    @pl.loop(fresh, b)
    def _(s):
        wait_twin(s)

    gpart[...] = jnp.zeros_like(gpart)

    @pl.loop(0, PIECES)
    def _(j):
        @pl.loop(fresh, b)
        def _(s):
            update(s, [j])

        apply_inverse(j)
        for d in range(1, bands):
            @pl.when(direct(d))
            def _():
                y_copy(b, j, d).start()

        out_copy(j).start()
        for k, (p, q) in enumerate(PAIRS):
            up, left = slice(p * rb, (p + 1) * rb), slice(q * rb, (q + 1) * rb)
            value = mm3(
                (own_hi[j, up], own_lo[j, up]), (own_hi[j, left], own_lo[j, left]), ((1,), (1,))
            )
            gpart[2 * k] += value[: rb // 2]
            gpart[2 * k + 1] += value[rb // 2 :]

    @pl.when(b == 0)
    def _():
        for j in range(PIECES):
            y_copy(b, j, last).start()

    mine = c * SHARE
    to_sib = remote(
        gpart.at[pl.ds((1 - c) * SHARE, SHARE)], gsib, twin_sem.at[0], twin_sem.at[1], (b, twin)
    )
    to_sib.start()
    lower_half = z < line // 2
    inward = jnp.where(lower_half, ga + 2, ga - 2)
    has_out = jnp.where(lower_half, z > 0, z < line - 1)
    outward = jnp.where(has_out, jnp.where(lower_half, ga - 2, ga + 2), inward)
    middle = jnp.where(lower_half, z == line // 2 - 1, z == line // 2)

    def in_copy(k):
        return remote(gpart.at[mine + k], gin.at[k], in_send.at[k], gin_recv.at[k], (b, inward))

    def cross_copy(k):
        return remote(gpart.at[mine + k], gcross.at[k], in_send.at[k], cross_recv.at[k], (b, inward))

    def back_copy(k):
        return remote(
            gout.at[mine + k], gout.at[mine + k], out_send.at[k], gout_recv.at[mine + k], (b, outward)
        )

    def share_copy(k, base):
        return remote(
            gout.at[base + k], gout.at[base + k], twin_send.at[k], gout_recv.at[base + k], (b, twin)
        )

    to_sib.wait_recv()

    def inward_leg(k):
        gpart[mine + k] += gsib[k]

        @pl.when(has_out)
        def _():
            in_copy(k).wait_recv()
            gpart[mine + k] += gin[k]

        @pl.when(middle)
        def _():
            cross_copy(k).start()

        @pl.when(jnp.logical_not(middle))
        def _():
            in_copy(k).start()

    def outward_leg(k):
        @pl.when(middle)
        def _():
            cross_copy(k).wait_recv()
            gout[mine + k] = gpart[mine + k] + gcross[k]

        @pl.when(jnp.logical_not(middle))
        def _():
            back_copy(k).wait_recv()

        @pl.when(has_out)
        def _():
            back_copy(k).start()

        share_copy(k, mine).start()

    lag = jnp.where(middle, 2, SHARE)

    @pl.loop(0, 2 * SHARE)
    def _(k):
        @pl.when(k < SHARE)
        def _():
            inward_leg(k)

        @pl.when(jnp.logical_and(k >= lag, k < SHARE + lag))
        def _():
            outward_leg(k - lag)

    theirs = (1 - c) * SHARE

    @pl.loop(0, SHARE)
    def _(k):
        share_copy(k, theirs).wait_recv()

    scale = 1.0 / (width * 2 * line)
    for k, (p, q) in enumerate(PAIRS):
        value = jnp.concatenate([gout[2 * k], gout[2 * k + 1]], axis=0) * scale
        g_ref[p * rb : (p + 1) * rb, q * rb : (q + 1) * rb] = value
        if p != q:
            g_ref[q * rb : (q + 1) * rb, p * rb : (p + 1) * rb] = value.T

    def drained(tile, turn, i, moves, send):
        s, live = tile(turn)
        s = jnp.clip(s, 0, last)
        for wide, on in sizes(s, c, i, live):
            @pl.when(jnp.logical_and(on, moves))
            def _():
                send(s, i, wide).wait_send()

            @pl.when(jnp.logical_and(on, s != z))
            def _():
                to_twin(s, i, wide).wait_send()

    for turn in range(bands - 1):
        @pl.loop(0, CHUNKS)
        def _(i):
            drained(right_tile, turn, i, z < line - 1, to_right)
            drained(left_tile, turn, i, z > 0, to_left)

    @pl.when(z <= b)
    def _():
        @pl.loop(0, CHUNKS)
        def _(i):
            for wide, on in sizes(z, c, i):
                @pl.when(on)
                def _():
                    to_twin(z, i, wide).wait_send()

    @pl.loop(0, PIECES)
    def _(j):
        for d in range(1, bands):
            @pl.when(direct(d))
            def _():
                y_copy(b, j, d).wait_send()

        @pl.when(b == 0)
        def _():
            y_copy(b, j, last).wait_send()

        out_copy(j).wait()

    to_sib.wait_send()

    @pl.loop(0, SHARE)
    def _(k):
        in_copy(k).wait_send()
        share_copy(k, mine).wait_send()

        @pl.when(has_out)
        def _():
            back_copy(k).wait_send()


def solution(mesh):
    bands, line = mesh.shape["band"], mesh.shape["ga"] // 2

    def local(psi, lower):
        nrows, width = psi.shape
        lw = lower.shape[1]
        w, rb = width // PIECES, nrows // ROWS
        vmem, dma = pltpu.VMEM, pltpu.SemaphoreType.DMA
        bf16 = jnp.bfloat16
        share = (SHARE, rb // 2, rb)
        return pl.pallas_call(
            functools.partial(kernel, bands, line),
            out_shape=(
                jax.ShapeDtypeStruct((nrows, width), F32),
                jax.ShapeDtypeStruct((nrows, nrows), F32),
            ),
            in_specs=[pl.BlockSpec(memory_space=pl.ANY)] * 2,
            out_specs=(pl.BlockSpec(memory_space=pl.ANY), pl.BlockSpec(memory_space=pltpu.VMEM)),
            scratch_shapes=[
                vmem((bands, 2, nrows, lw), F32),
                vmem((PIECES, nrows, w), F32),
                vmem((bands - 1, PIECES, nrows, w), F32),
                vmem((PIECES, nrows, w), F32),
                vmem((PIECES, nrows, w), bf16),
                vmem((PIECES, nrows, w), bf16),
                vmem((PIECES, nrows, w), bf16),
                vmem((PIECES, nrows, w), bf16),
                vmem((nrows, nrows), F32),
                vmem((nrows, nrows), bf16),
                vmem((nrows, nrows), bf16),
                vmem((nrows // 2, nrows // 2), F32),
                vmem((2 * SHARE, rb // 2, rb), F32),
                vmem(share, F32),
                vmem(share, F32),
                vmem(share, F32),
                vmem((2 * SHARE, rb // 2, rb), F32),
                dma((bands, 2, CHUNKS)),
                dma((bands, CHUNKS)),
                dma((bands, CHUNKS)),
                dma((bands, CHUNKS)),
                dma((bands - 1, PIECES)),
                dma((bands - 1, PIECES)),
                dma((PIECES,)),
                dma((PIECES,)),
                dma((1,)),
                dma((2,)),
                dma((SHARE,)),
                dma((SHARE,)),
                dma((SHARE,)),
                dma((2 * SHARE,)),
                dma((SHARE,)),
                dma((SHARE,)),
            ],
            compiler_params=pltpu.CompilerParams(
                collective_id=0, has_side_effects=True, vmem_limit_bytes=63 * 1024 * 1024
            ),
        )(psi, lower)

    return jax.shard_map(
        local,
        mesh=mesh,
        in_specs=(P("band", "ga"), P("band", "ga")),
        out_specs=(P("band", "ga"), P("band", None)),
        check_vma=False,
    )
```
